32 devices in a mesh: dp: 16 (over z, x, core), tensor: 2 (over y).
Axes of the slice: x: 2, y: 2, z: 4, core: 2. Of those that a mesh axis runs over, the one named last changes fastest.
Arguments:
- x_in: bfloat16 [16, 2, 1024, 768], P(None, 'tensor', 'dp'), may hold values from -6 to 6
- cotangent: bfloat16 [16, 2, 1024, 768], P(None, 'tensor', 'dp'), may hold values from -6 to 6
- lengths: int32 [16], replicated, may hold values from 1 to 2048, 24576 in all
- dealing: int32 [16], replicated, may hold values from 0 to 15, each once
- w_qkv: float32 [768, 3, 768], P('dp', None, 'tensor'), may hold values from -0.21875 to 0.21875
- w_out: float32 [768, 768], P('dp', 'tensor'), may hold values from -1.75 to 1.75
- w_in: float32 [768, 3072], P('dp', 'tensor'), may hold values from -0.21875 to 0.21875
- w_ffo: float32 [768, 3072], P('dp', 'tensor'), may hold values from -0.109375 to 0.109375
- b_qv: float32 [2, 768], P(None, 'tensor'), may hold values from -3 to 3
- b_out: float32 [768], replicated, may hold values from -3 to 3
- b_in: float32 [3072], P('tensor'), may hold values from -3 to 3
- b_ffo: float32 [768], replicated, may hold values from -3 to 3
- ln1_gain: float32 [768], replicated, may hold values from 0.1 to 1.9
- ln1_bias: float32 [768], replicated, may hold values from -3 to 3
- ln2_gain: float32 [768], replicated, may hold values from 0.1 to 1.9
- ln2_bias: float32 [768], replicated, may hold values from -3 to 3
Outputs:
- out: bfloat16 [16, 2, 1024, 768], P(None, 'tensor', 'dp')
- grad_in: bfloat16 [16, 2, 1024, 768], P(None, 'tensor', 'dp')
- grad_w_qkv: float32 [768, 3, 768], P('dp', None, 'tensor')
- grad_w_out: float32 [768, 768], P('dp', 'tensor')
- grad_w_in: float32 [768, 3072], P('dp', 'tensor')
- grad_w_ffo: float32 [768, 3072], P('dp', 'tensor')
- grad_b_qv: float32 [2, 768], P(None, 'tensor')
- grad_b_out: float32 [768], replicated
- grad_b_in: float32 [3072], P('tensor')
- grad_b_ffo: float32 [768], replicated
- grad_ln1_gain: float32 [768], replicated
- grad_ln1_bias: float32 [768], replicated
- grad_ln2_gain: float32 [768], replicated
- grad_ln2_bias: float32 [768], replicated
The draws below stay inside these ranges and needn't reach their ends.
Inputs may be any that keep to these rules, and one draw needn't show every extreme that they name: Slot j holds lengths[j] tokens of its sequence and padding after them; some slot is full, 2048 tokens. Sequence s goes to slot dealing[s]; every slot gets one sequence.
All inputs are finite; a program needn't handle non-finite values.
Results may differ from the reference program's by a relative error of at most 0.018.
Values may be sent and summed in bfloat16 or wider, within the bound.
A program may use at most 192 MiB of HBM per device.

```python
import math
import jax
import jax.numpy as jnp
import numpy as np
from jax import lax

HEADS = 12
HEAD_DIM = 64
FF = 3072
D = 768
SEQ_LEN = 2048
SEQS = 16
N_TENSOR = 2


def block_scale(key, shape, shards, smallest, top_value):
    def one(position, parts):
        steps = jax.random.uniform(jax.random.fold_in(jax.random.fold_in(key, 6), position), (parts,), jnp.float32, smallest / len(shards), top_value / len(shards))
        return jnp.repeat(jnp.exp(steps), shape[position] // parts).reshape((-1,) + (1,) * (len(shape) - position - 1))

    gain = one(*shards[0])
    for cut in shards[1:]:
        gain = gain * one(*cut)
    return gain


def split_up(amount, total, reach, slope):
    weights = [(1 << 20) // math.isqrt(standing ** slope) + 1 for standing in range(2, amount + 1)]
    spare, holding = total - reach - (amount - 1), [1] * (amount - 1)
    while spare > 0:
        movable = [i for i in range(amount - 1) if holding[i] < reach]
        pool, budget = sum([weights[i] for i in movable]), spare
        for i in movable:
            more = min(reach - holding[i], max(1, budget * weights[i] // pool), spare)
            holding[i] = holding[i] + more
            spare = spare - more
    return np.array([reach] + holding)


def uneven_parts(rng, amount, total, most, lean):
    if amount == 2:
        one = jax.random.randint(rng, (), max(1, total - most), min(most, total - 1) + 1)
        return jnp.stack([one, total - one])
    sizes = jnp.asarray(split_up(amount, total, most, lean), jnp.int32)
    couples = (amount - 1) // 2
    source_of, receiver = sizes[1:1 + 2 * couples:2], sizes[2:2 + 2 * couples:2]
    room = jnp.minimum(source_of - 1, most - receiver)
    passed = jax.random.randint(jax.random.fold_in(rng, 1), (couples,), 0, 1 << 20) % (room + 1)
    sizes = sizes.at[1:1 + 2 * couples:2].set(source_of - passed).at[2:2 + 2 * couples:2].set(receiver + passed)
    return sizes[jax.random.permutation(jax.random.fold_in(rng, 2), amount)]


def normal_values(stream_key, extent, scale, limit, pieces=(), kind=jnp.bfloat16):
    entries = scale * jax.random.normal(stream_key, extent, jnp.float32)
    if pieces:
        entries = entries * block_scale(stream_key, extent, pieces, -0.22, 0.18)
    return jnp.clip(entries, -limit, limit).astype(kind)


def setup_inputs(seed: int = 0) -> dict:
    keys = jax.random.split(jax.random.key(seed), 17)
    x_in = normal_values(keys[0], (SEQS, N_TENSOR, SEQ_LEN // N_TENSOR, D), 1.0, 6.0, ((1, 2), (2, 16)))
    cotangent = normal_values(keys[1], (SEQS, N_TENSOR, SEQ_LEN // N_TENSOR, D), 1.0, 6.0, ((1, 2), (2, 16)))
    lengths = uneven_parts(keys[2], SEQS, SEQS * SEQ_LEN * 3 // 4, SEQ_LEN, 1).astype(jnp.int32)
    dealing = jax.random.permutation(keys[3], SEQS).astype(jnp.int32)
    w_qkv = normal_values(keys[4], (D, 3, D), D ** -0.5, 0.21875, ((0, 16), (2, 2)), jnp.float32)
    w_out = normal_values(keys[5], (D, D), (D // 64) ** -0.5, 1.75, ((0, 16), (1, 2)), jnp.float32)
    w_in = normal_values(keys[6], (D, FF), D ** -0.5, 0.21875, ((0, 16), (1, 2)), jnp.float32)
    w_ffo = normal_values(keys[7], (D, FF), FF ** -0.5, 0.109375, ((0, 16), (1, 2)), jnp.float32)
    b_qv = normal_values(keys[8], (2, D), 0.5, 3.0, ((1, 2),), jnp.float32)
    b_out = normal_values(keys[9], (D,), 0.5, 3.0, (), jnp.float32)
    b_in = normal_values(keys[10], (FF,), 0.5, 3.0, ((0, 2),), jnp.float32)
    b_ffo = normal_values(keys[11], (D,), 0.5, 3.0, (), jnp.float32)
    ln1_gain = jnp.clip(1.0 + 0.18 * jax.random.normal(keys[12], (D,), jnp.float32), 0.1, 1.9)
    ln1_bias = normal_values(keys[13], (D,), 0.5, 3.0, (), jnp.float32)
    ln2_gain = jnp.clip(1.0 + 0.18 * jax.random.normal(keys[14], (D,), jnp.float32), 0.1, 1.9)
    ln2_bias = normal_values(keys[15], (D,), 0.5, 3.0, (), jnp.float32)
    return dict(x_in=x_in, cotangent=cotangent, lengths=lengths, dealing=dealing, w_qkv=w_qkv, w_out=w_out, w_in=w_in, w_ffo=w_ffo, b_qv=b_qv, b_out=b_out, b_in=b_in, b_ffo=b_ffo, ln1_gain=ln1_gain, ln1_bias=ln1_bias, ln2_gain=ln2_gain, ln2_bias=ln2_bias)


HIGHEST = lax.Precision.HIGHEST

@jax.custom_vjp
def low(v):
    return lax.optimization_barrier(v.astype(jnp.bfloat16)).astype(jnp.float32)

@jax.custom_vjp
def low_back(v):
    return v

def low_keep(v):
    return (low(v), None)

def low_pass(kept, grad):
    return (grad,)

def back_keep(v):
    return (v, None)

def back_low(kept, grad):
    return (low(grad),)
low.defvjp(low_keep, low_pass)
low_back.defvjp(back_keep, back_low)

def layer_norm(values, norm_gain, norm_shift):
    centre = lax.optimization_barrier(jnp.mean(values, axis=-1, keepdims=True))
    centred = values - centre
    spread = lax.optimization_barrier(jnp.mean(centred * centred, axis=-1, keepdims=True))
    return centred * lax.rsqrt(spread + 1e-06) * norm_gain + norm_shift

def attend(query_rows, key_rows, value_rows, key_valid):
    scores = jnp.einsum('qhe,khe->hqk', query_rows, key_rows, precision=HIGHEST) * HEAD_DIM ** (-0.5)
    scores = jnp.where(key_valid[None, None, :], low_back(scores), -jnp.inf)
    weights = jax.nn.softmax(scores, axis=-1)
    return jnp.einsum('hqk,khe->qhe', low(weights), value_rows, precision=HIGHEST)

def sequence_layer(weights_low, small_params, tokens, used_keys):
    qkv_weight, out_weight, in_weight, ffo_weight = weights_low
    qv_bias, out_bias, in_bias, ffo_bias, gain_one, shift_one, gain_two, shift_two = small_params
    key_valid = jnp.arange(SEQ_LEN) < used_keys
    projected = jnp.einsum('ld,dce->cle', tokens, qkv_weight, precision=HIGHEST)
    query_all = low(low_back(projected[0] + qv_bias[0])).reshape(SEQ_LEN, HEADS, HEAD_DIM)
    key_all = low(low_back(projected[1])).reshape(SEQ_LEN, HEADS, HEAD_DIM)
    value_all = low(low_back(projected[2] + qv_bias[1])).reshape(SEQ_LEN, HEADS, HEAD_DIM)
    block_rows = min(512, SEQ_LEN)
    query_blocks = query_all.reshape(SEQ_LEN // block_rows, block_rows, HEADS, HEAD_DIM)

    def one_block(query_rows):
        return attend(query_rows, key_all, value_all, key_valid)
    mixed_heads = lax.map(jax.checkpoint(one_block), query_blocks).reshape(SEQ_LEN, D)
    mixed_heads = low(low_back(mixed_heads))
    branch = low_back(jnp.einsum('le,de->ld', mixed_heads, out_weight, precision=HIGHEST))
    first_norm = layer_norm(tokens + branch + out_bias, gain_one, shift_one)
    hidden = low_back(jnp.einsum('ld,df->lf', low(first_norm), in_weight, precision=HIGHEST) + in_bias)
    active = low(jax.nn.gelu(hidden, approximate=False))
    branch_two = low_back(jnp.einsum('lf,df->ld', active, ffo_weight, precision=HIGHEST))
    return layer_norm(first_norm + branch_two + ffo_bias, gain_two, shift_two)

def reference(x_in, cotangent, lengths, dealing, w_qkv, w_out, w_in, w_ffo, b_qv, b_out, b_in, b_ffo, ln1_gain, ln1_bias, ln2_gain, ln2_bias):
    seq_lengths = jnp.take(lengths, dealing, axis=0).astype(jnp.int32)
    inputs = x_in.astype(jnp.float32).reshape(SEQS, SEQ_LEN, D)
    upstream = cotangent.astype(jnp.float32).reshape(SEQS, SEQ_LEN, D)
    params = (w_qkv, w_out, w_in, w_ffo, b_qv, b_out, b_in, b_ffo, ln1_gain, ln1_bias, ln2_gain, ln2_bias)

    def forward(all_params, all_inputs):
        weights_low = (low(all_params[0]), low(all_params[1]), low(all_params[2]), low(all_params[3]))
        small_params = all_params[4:]

        def one_sequence(sequence_item):
            return sequence_layer(weights_low, small_params, sequence_item[0], sequence_item[1])
        return lax.map(jax.checkpoint(one_sequence), (all_inputs, seq_lengths))
    outputs, pullback = jax.vjp(forward, params, inputs)
    param_grads, input_grads = pullback(upstream)
    layout = (SEQS, N_TENSOR, SEQ_LEN // N_TENSOR, D)
    return (outputs.reshape(layout).astype(jnp.bfloat16), input_grads.reshape(layout).astype(jnp.bfloat16), param_grads[0], param_grads[1], param_grads[2], param_grads[3], param_grads[4], param_grads[5], param_grads[6], param_grads[7], param_grads[8], param_grads[9], param_grads[10], param_grads[11])
```

```python
import functools

import jax
import jax.numpy as jnp
from jax import lax
from jax.experimental import pallas as pl
from jax.experimental.pallas import tpu as pltpu
from jax.sharding import PartitionSpec as P

LOG2E = 1.4426950408889634
MASKED = -1e30
HEAD_DIM = 64
PAIR = 2 * HEAD_DIM


def contract_last(a, b):
    return lax.dot_general(a, b, (((1,), (1,)), ((), ())), preferred_element_type=jnp.float32)


def lane_iota(shape):
    return lax.broadcasted_iota(jnp.int32, shape, len(shape) - 1)


def attn_fwd_kernel(scale, len_ref, q_ref, k_ref, v_ref, o_ref, lse_ref, kx, vx):
    keys = k_ref.shape[0]
    rows = q_ref.shape[0]

    @pl.when(pl.program_id(1) == 0)
    def _():
        lanes = lane_iota((keys, PAIR))
        valid = lax.broadcasted_iota(jnp.int32, (keys, PAIR), 0) < len_ref[0]
        bias = jnp.where(valid, 0.0, MASKED)
        k2 = k_ref[...].astype(jnp.float32)
        v2 = v_ref[...].astype(jnp.float32)
        for h in range(2):
            mine = (lanes // HEAD_DIM) == h
            spare = lanes == (1 - h) * HEAD_DIM
            kx[h] = jnp.where(mine, k2, jnp.where(spare, bias, 0.0)).astype(jnp.bfloat16)
            vx[h] = jnp.where(mine, v2, 1.0).astype(jnp.bfloat16)

    lanes = lane_iota((rows, PAIR))
    q2 = q_ref[...].astype(jnp.float32)
    low = lanes < HEAD_DIM
    sums, tops = [], []
    for h in range(2):
        mine = (lanes // HEAD_DIM) == h
        spare = lanes == (1 - h) * HEAD_DIM
        qx = jnp.where(mine, q2, jnp.where(spare, 1.0, 0.0)).astype(jnp.bfloat16)
        s = contract_last(qx, kx[h])
        top = jnp.max(s, axis=1, keepdims=True)
        p = jnp.exp2(s * scale - top * scale).astype(jnp.bfloat16)
        sums.append(jnp.dot(p, vx[h], preferred_element_type=jnp.float32))
        tops.append(top * scale)
    num = jnp.where(low, sums[0], sums[1])
    den = pltpu.roll(jnp.where(low, sums[1], sums[0]), HEAD_DIM, 1)
    o_ref[...] = (num / den).astype(jnp.bfloat16)
    lse_ref[...] = jnp.where(low, tops[0], tops[1]) + jnp.log2(den)


def attn_fwd(length, q, kv, block):
    rows, width = q.shape
    keys = kv.shape[0]
    pairs = width // PAIR
    return pl.pallas_call(
        functools.partial(attn_fwd_kernel, LOG2E * HEAD_DIM ** -0.5),
        grid_spec=pltpu.PrefetchScalarGridSpec(
            num_scalar_prefetch=1,
            grid=(pairs, rows // block),
            in_specs=[
                pl.BlockSpec((block, PAIR), lambda p, i, n: (i, p)),
                pl.BlockSpec((keys, PAIR), lambda p, i, n: (0, p)),
                pl.BlockSpec((keys, PAIR), lambda p, i, n: (0, pairs + p)),
            ],
            out_specs=[
                pl.BlockSpec((block, PAIR), lambda p, i, n: (i, p)),
                pl.BlockSpec((block, PAIR), lambda p, i, n: (i, p)),
            ],
            scratch_shapes=[
                pltpu.VMEM((2, keys, PAIR), jnp.bfloat16),
                pltpu.VMEM((2, keys, PAIR), jnp.bfloat16),
            ],
        ),
        out_shape=[
            jax.ShapeDtypeStruct((rows, width), jnp.bfloat16),
            jax.ShapeDtypeStruct((rows, width), jnp.float32),
        ],
        name="attn_fwd",
        cost_estimate=pl.CostEstimate(flops=4 * rows * keys * width * 4, bytes_accessed=10_000_000, transcendentals=rows * keys * width // 64),
    )(length, q, kv, kv)


def split3(x):
    a = x.astype(jnp.bfloat16).astype(jnp.float32)
    b = (x - a).astype(jnp.bfloat16).astype(jnp.float32)
    return a, b, x - a - b


def attn_bwd_kernel(scale, len_ref, q_ref, k_ref, v_ref, o_ref, lse_ref, g_ref, dq_ref, dk_ref, dv_ref, qx, gx, qz, gz, dqt):
    rows = q_ref.shape[0]
    keys = k_ref.shape[0]
    c = pl.program_id(1)

    @pl.when(c == 0)
    def _():
        lanes = lane_iota((rows, PAIR))
        q2 = q_ref[...].astype(jnp.float32)
        g2 = g_ref[...].astype(jnp.float32)
        go = g2 * o_ref[...].astype(jnp.float32)
        other = -pltpu.roll(lse_ref[...], HEAD_DIM, 1) * (1.0 / scale)
        a, b, d = split3(other)
        for h in range(2):
            mine = (lanes // HEAD_DIM) == h
            base = (1 - h) * HEAD_DIM
            delta = -jnp.sum(jnp.where(mine, go, 0.0), axis=1, keepdims=True)
            da, db, dd = split3(delta)
            ext = jnp.where(lanes == base, a, jnp.where(lanes == base + 1, b, jnp.where(lanes == base + 2, d, jnp.where(lanes == base + 3, 1.0, 0.0))))
            qx[h] = jnp.where(mine, q2, ext).astype(jnp.bfloat16)
            qz[h] = jnp.where(mine, q2, 0.0).astype(jnp.bfloat16)
            ext = jnp.where(lanes == base, da, jnp.where(lanes == base + 1, db, jnp.where(lanes == base + 2, dd, 0.0)))
            gx[h] = jnp.where(mine, g2, ext).astype(jnp.bfloat16)
            gz[h] = jnp.where(mine, g2, 0.0).astype(jnp.bfloat16)
        dqt[...] = jnp.zeros_like(dqt)

    lanes = lane_iota((keys, PAIR))
    valid = lax.broadcasted_iota(jnp.int32, (keys, PAIR), 0) + c * keys < len_ref[0]
    bias = jnp.where(valid, 0.0, MASKED)
    k2 = k_ref[...].astype(jnp.float32)
    v2 = v_ref[...].astype(jnp.float32)
    kt = k2.T.astype(jnp.bfloat16)
    dv = None
    dk = None
    for h in range(2):
        mine = (lanes // HEAD_DIM) == h
        base = (1 - h) * HEAD_DIM
        ones = jnp.where((lanes >= base) & (lanes < base + 3), 1.0, 0.0)
        kx = jnp.where(mine, k2, jnp.where(lanes == base + 3, bias, ones)).astype(jnp.bfloat16)
        vx = jnp.where(mine, v2, ones).astype(jnp.bfloat16)
        s = contract_last(kx, qx[h])
        p = jnp.exp2(s * scale)
        da = contract_last(vx, gx[h])
        ds = (p * da).astype(jnp.bfloat16)
        dv_h = jnp.dot(p.astype(jnp.bfloat16), gz[h], preferred_element_type=jnp.float32)
        dk_h = jnp.dot(ds, qz[h], preferred_element_type=jnp.float32)
        dv = dv_h if dv is None else dv + dv_h
        dk = dk_h if dk is None else dk + dk_h
        half = pl.ds(h * HEAD_DIM, HEAD_DIM)
        dqt[half, :] += jnp.dot(kt[h * HEAD_DIM : (h + 1) * HEAD_DIM], ds, preferred_element_type=jnp.float32)
    root = HEAD_DIM ** -0.5
    dk_ref[...] = (dk * root).astype(jnp.bfloat16)
    dv_ref[...] = dv.astype(jnp.bfloat16)

    @pl.when(c == pl.num_programs(1) - 1)
    def _():
        dq_ref[...] = (dqt[...] * root).T.astype(jnp.bfloat16)


def attn_bwd(length, q, kv, o, lse, g, block):
    rows, width = q.shape
    keys = kv.shape[0]
    pairs = width // PAIR
    whole = pl.BlockSpec((rows, PAIR), lambda p, i, n: (0, p))
    part = pl.BlockSpec((block, PAIR), lambda p, i, n: (i, p))
    late = pl.BlockSpec((block, PAIR), lambda p, i, n: (i, pairs + p))
    out = pl.pallas_call(
        functools.partial(attn_bwd_kernel, LOG2E * HEAD_DIM ** -0.5),
        grid_spec=pltpu.PrefetchScalarGridSpec(
            num_scalar_prefetch=1,
            grid=(pairs, keys // block),
            in_specs=[whole, part, late, whole, whole, whole],
            out_specs=[whole, part, part],
            scratch_shapes=[pltpu.VMEM((2, rows, PAIR), jnp.bfloat16)] * 4
            + [pltpu.VMEM((PAIR, rows), jnp.float32)],
        ),
        out_shape=[
            jax.ShapeDtypeStruct((rows, width), jnp.bfloat16),
            jax.ShapeDtypeStruct((keys, width), jnp.bfloat16),
            jax.ShapeDtypeStruct((keys, width), jnp.bfloat16),
        ],
        name="attn_bwd",
        cost_estimate=pl.CostEstimate(flops=10 * rows * keys * width * 4, bytes_accessed=20_000_000, transcendentals=rows * keys * width // 64),
    )(length, q, kv, kv, o, lse, g)
    return out


def contract_first(a, b):
    return lax.dot_general(a, b, (((0,), (0,)), ((), ())), preferred_element_type=jnp.float32)


def dense(a, b):
    return jnp.dot(a, b, preferred_element_type=jnp.float32)


def norm_forward(values, norm_gain, norm_shift):
    centre = jnp.mean(values, axis=-1, keepdims=True)
    centred = values - centre
    inverse = lax.rsqrt(jnp.mean(centred * centred, axis=-1, keepdims=True) + 1e-06)
    normed = centred * inverse
    return (normed * norm_gain + norm_shift, normed, inverse)


def norm_backward(upstream, normed, inverse, norm_gain):
    scaled = upstream * norm_gain
    back_rows = inverse * (
        scaled
        - jnp.mean(scaled, axis=-1, keepdims=True)
        - normed * jnp.mean(scaled * normed, axis=-1, keepdims=True)
    )
    return (back_rows, jnp.sum(upstream * normed, axis=0), jnp.sum(upstream, axis=0))


def gelu_slope(values):
    return (
        0.5 * (1.0 + lax.erf(values * 0.7071067811865476))
        + values * jnp.exp(-0.5 * values * values) * 0.3989422804014327
    )


def deal(blocks):
    out = lax.all_to_all(blocks, "dp", split_axis=0, concat_axis=0, tiled=True)
    return out.reshape(-1, out.shape[-1])


def undeal(rows):
    blocks = rows.reshape(lax.axis_size("dp"), -1, rows.shape[-1])
    return lax.all_to_all(blocks, "dp", split_axis=0, concat_axis=0, tiled=True)[:, None]


def gather_weight(weight):
    low = lax.all_gather(weight.astype(jnp.bfloat16), "tensor", axis=weight.ndim - 1, tiled=True)
    return lax.all_gather(low, "dp", axis=0, tiled=True)


def scatter_weight(grad):
    part = lax.psum_scatter(grad.astype(jnp.bfloat16), "dp", scatter_dimension=0, tiled=True)
    return lax.psum_scatter(
        part.astype(jnp.float32), "tensor", scatter_dimension=grad.ndim - 1, tiled=True
    )


def per_device(
    x_in, cotangent, lengths, dealing, w_qkv, w_out, w_in, w_ffo,
    b_qv, b_out, b_in, b_ffo, ln1_gain, ln1_bias, ln2_gain, ln2_bias,
):
    low = jnp.bfloat16
    tensor_index = lax.axis_index("tensor")
    width = x_in.shape[-1]
    length = lengths[dealing[lax.axis_index("dp")]][None].astype(jnp.int32)
    qkv_weight = gather_weight(w_qkv)
    biases = lax.all_gather(
        jnp.concatenate([b_qv.reshape(-1), b_in]), "tensor", axis=0, tiled=False
    )
    split = 2 * b_qv.shape[1]
    qv_bias = biases[:, :split].reshape(-1, 2, b_qv.shape[1]).transpose(1, 0, 2).reshape(2, -1)
    in_bias = biases[:, split:].reshape(-1)
    tokens_half = deal(x_in[:, 0])
    half_rows = tokens_half.shape[0]
    tokens_full = lax.all_gather(tokens_half, "tensor", axis=0, tiled=True)
    out_weight = gather_weight(w_out)
    in_weight = gather_weight(w_in)
    ffo_weight = gather_weight(w_ffo)
    q_weight = qkv_weight[:, 0]
    kv_weight = qkv_weight[:, 1:].reshape(width, -1)
    query = (dense(tokens_half, q_weight) + qv_bias[0]).astype(low)
    kv_bias = jnp.concatenate([jnp.zeros((width,), jnp.float32), qv_bias[1]])
    keyval = (dense(tokens_full, kv_weight) + kv_bias).astype(low)
    mixed, totals = attn_fwd(length, query, keyval, 256)
    attn_half = contract_last(mixed, out_weight)
    first_norm, normed_one, inverse_one = norm_forward(
        tokens_half.astype(jnp.float32) + attn_half + b_out, ln1_gain, ln1_bias
    )
    first_low = first_norm.astype(low)
    hidden = dense(first_low, in_weight) + in_bias
    active = jax.nn.gelu(hidden, approximate=False).astype(low)
    result, normed_two, inverse_two = norm_forward(
        first_norm + contract_last(active, ffo_weight) + b_ffo, ln2_gain, ln2_bias
    )
    output_grad = deal(cotangent[:, 0]).astype(jnp.float32)
    final_grad, gain_two_grad, shift_two_grad = norm_backward(
        output_grad, normed_two, inverse_two, ln2_gain
    )
    ffo_bias_grad = jnp.sum(final_grad, axis=0)
    final_low = final_grad.astype(low)
    ffo_sum = scatter_weight(contract_first(final_low, active))
    hidden_grad = (dense(final_low, ffo_weight) * gelu_slope(hidden)).astype(low)
    in_sum = scatter_weight(contract_first(first_low, hidden_grad))
    in_bias_grad = jnp.sum(hidden_grad.astype(jnp.float32), axis=0)
    first_grad = final_grad + contract_last(hidden_grad, in_weight)
    resid_grad, gain_one_grad, shift_one_grad = norm_backward(
        first_grad, normed_one, inverse_one, ln1_gain
    )
    out_bias_grad = jnp.sum(resid_grad, axis=0)
    resid_low = resid_grad.astype(low)
    out_sum = scatter_weight(contract_first(resid_low, mixed))
    mixed_grad = dense(resid_low, out_weight).astype(low)
    dq, dk, dv = attn_bwd(length, query, keyval, mixed, totals, mixed_grad, 512)
    q_bias_grad = jnp.sum(dq.astype(jnp.float32), axis=0)
    v_bias_grad = jnp.sum(dv.astype(jnp.float32), axis=0)
    qkv_grad = jnp.stack(
        [
            contract_first(tokens_half, dq),
            contract_first(tokens_full, dk),
            contract_first(tokens_full, dv),
        ],
        axis=1,
    )
    qkv_sum = scatter_weight(qkv_grad)
    shared = contract_last(dk, qkv_weight[:, 1]) + contract_last(dv, qkv_weight[:, 2])
    own = lax.psum_scatter(shared.astype(low), "tensor", scatter_dimension=0, tiled=True)
    input_grad = resid_grad + contract_last(dq, q_weight) + own.astype(jnp.float32)
    terms = jnp.concatenate(
        [
            out_bias_grad, ffo_bias_grad, gain_one_grad, shift_one_grad,
            gain_two_grad, shift_two_grad, q_bias_grad, v_bias_grad, in_bias_grad,
        ]
    )
    sums = lax.psum(terms, ("dp", "tensor"))
    norm_sums = sums[: 6 * width].reshape(6, width)
    qv_sums = sums[6 * width : 8 * width].reshape(2, width)
    share = b_qv.shape[1]
    qv_share = lax.dynamic_slice_in_dim(qv_sums, tensor_index * share, share, 1)
    share = b_in.shape[0]
    in_share = lax.dynamic_slice_in_dim(sums[8 * width :], tensor_index * share, share, 0)
    return (
        undeal(result.astype(low)),
        undeal(input_grad.astype(low)),
        qkv_sum,
        out_sum,
        in_sum,
        ffo_sum,
        qv_share,
        norm_sums[0],
        in_share,
        norm_sums[1],
        norm_sums[2],
        norm_sums[3],
        norm_sums[4],
        norm_sums[5],
    )


def solution(mesh):
    tokens = P(None, "tensor", "dp", None)
    return jax.shard_map(
        per_device,
        mesh=mesh,
        in_specs=(
            tokens, tokens, P(), P(),
            P("dp", None, "tensor"), P("dp", "tensor"), P("dp", "tensor"), P("dp", "tensor"),
            P(None, "tensor"), P(), P("tensor"), P(), P(), P(), P(), P(),
        ),
        out_specs=(
            tokens, tokens,
            P("dp", None, "tensor"), P("dp", "tensor"), P("dp", "tensor"), P("dp", "tensor"),
            P(None, "tensor"), P(), P("tensor"), P(), P(), P(), P(), P(),
        ),
        check_vma=False,
    )
```

```python
import functools

import jax
import jax.numpy as jnp
from jax import lax
from jax.experimental import pallas as pl
from jax.experimental.pallas import tpu as pltpu
from jax.sharding import PartitionSpec as P


LOG2E = 1.4426950408889634
MASKED = -1e30
HEAD_DIM = 64
PAIR = 2 * HEAD_DIM


def contract_last(a, b):
    return lax.dot_general(a, b, (((1,), (1,)), ((), ())), preferred_element_type=jnp.float32)


def lane_iota(shape):
    return lax.broadcasted_iota(jnp.int32, shape, len(shape) - 1)


def key_places(rows, start, total, place_ref):
    spots = lax.broadcasted_iota(jnp.int32, (rows, PAIR), 0) + (start + place_ref[1])
    return jnp.where(spots >= total, spots - total, spots)


def attn_fwd_kernel(scale, len_ref, q_ref, k_ref, v_ref, o_ref, lse_ref, kx, vx):
    keys = k_ref.shape[0]
    rows = q_ref.shape[0]

    @pl.when(pl.program_id(1) == 0)
    def _():
        lanes = lane_iota((keys, PAIR))
        valid = key_places(keys, 0, keys, len_ref) < len_ref[0]
        bias = jnp.where(valid, 0.0, MASKED)
        k2 = k_ref[...].astype(jnp.float32)
        v2 = v_ref[...].astype(jnp.float32)
        for h in range(2):
            mine = (lanes // HEAD_DIM) == h
            spare = lanes == (1 - h) * HEAD_DIM
            kx[h] = jnp.where(mine, k2, jnp.where(spare, bias, 0.0)).astype(jnp.bfloat16)
            vx[h] = jnp.where(mine, v2, 1.0).astype(jnp.bfloat16)

    lanes = lane_iota((rows, PAIR))
    q2 = q_ref[...].astype(jnp.float32)
    low = lanes < HEAD_DIM
    sums, tops = [], []
    for h in range(2):
        mine = (lanes // HEAD_DIM) == h
        spare = lanes == (1 - h) * HEAD_DIM
        qx = jnp.where(mine, q2, jnp.where(spare, 1.0, 0.0)).astype(jnp.bfloat16)
        s = contract_last(qx, kx[h])
        top = jnp.max(s, axis=1, keepdims=True)
        p = jnp.exp2(s * scale - top * scale).astype(jnp.bfloat16)
        sums.append(jnp.dot(p, vx[h], preferred_element_type=jnp.float32))
        tops.append(top * scale)
    num = jnp.where(low, sums[0], sums[1])
    den = pltpu.roll(jnp.where(low, sums[1], sums[0]), HEAD_DIM, 1)
    o_ref[...] = (num / den).astype(jnp.bfloat16)
    lse_ref[...] = jnp.where(low, tops[0], tops[1]) + jnp.log2(den)


def attn_fwd(length, q, kv, block):
    rows, width = q.shape
    keys = kv.shape[0]
    pairs = width // PAIR
    return pl.pallas_call(
        functools.partial(attn_fwd_kernel, LOG2E * HEAD_DIM ** -0.5),
        grid_spec=pltpu.PrefetchScalarGridSpec(
            num_scalar_prefetch=1,
            grid=(pairs, rows // block),
            in_specs=[
                pl.BlockSpec((block, PAIR), lambda p, i, n: (i, p)),
                pl.BlockSpec((keys, PAIR), lambda p, i, n: (0, p)),
                pl.BlockSpec((keys, PAIR), lambda p, i, n: (0, pairs + p)),
            ],
            out_specs=[
                pl.BlockSpec((block, PAIR), lambda p, i, n: (i, p)),
                pl.BlockSpec((block, PAIR), lambda p, i, n: (i, p)),
            ],
            scratch_shapes=[
                pltpu.VMEM((2, keys, PAIR), jnp.bfloat16),
                pltpu.VMEM((2, keys, PAIR), jnp.bfloat16),
            ],
        ),
        out_shape=[
            jax.ShapeDtypeStruct((rows, width), jnp.bfloat16),
            jax.ShapeDtypeStruct((rows, width), jnp.float32),
        ],
        name="attn_fwd",
        cost_estimate=pl.CostEstimate(flops=4 * rows * keys * width * 4, bytes_accessed=10_000_000, transcendentals=rows * keys * width // 64),
    )(length, q, kv, kv)


def split3(x):
    a = x.astype(jnp.bfloat16).astype(jnp.float32)
    b = (x - a).astype(jnp.bfloat16).astype(jnp.float32)
    return a, b, x - a - b


def attn_bwd_kernel(scale, len_ref, q_ref, k_ref, v_ref, o_ref, lse_ref, g_ref, dq_ref, dk_ref, dv_ref, qx, gx, qz, gz, dqt):
    rows = q_ref.shape[0]
    keys = k_ref.shape[0]
    c = pl.program_id(1)

    @pl.when(c == 0)
    def _():
        lanes = lane_iota((rows, PAIR))
        q2 = q_ref[...].astype(jnp.float32)
        g2 = g_ref[...].astype(jnp.float32)
        go = g2 * o_ref[...].astype(jnp.float32)
        other = -pltpu.roll(lse_ref[...], HEAD_DIM, 1) * (1.0 / scale)
        a, b, d = split3(other)
        for h in range(2):
            mine = (lanes // HEAD_DIM) == h
            base = (1 - h) * HEAD_DIM
            delta = -jnp.sum(jnp.where(mine, go, 0.0), axis=1, keepdims=True)
            da, db, dd = split3(delta)
            ext = jnp.where(lanes == base, a, jnp.where(lanes == base + 1, b, jnp.where(lanes == base + 2, d, jnp.where(lanes == base + 3, 1.0, 0.0))))
            qx[h] = jnp.where(mine, q2, ext).astype(jnp.bfloat16)
            qz[h] = jnp.where(mine, q2, 0.0).astype(jnp.bfloat16)
            ext = jnp.where(lanes == base, da, jnp.where(lanes == base + 1, db, jnp.where(lanes == base + 2, dd, 0.0)))
            gx[h] = jnp.where(mine, g2, ext).astype(jnp.bfloat16)
            gz[h] = jnp.where(mine, g2, 0.0).astype(jnp.bfloat16)
        dqt[...] = jnp.zeros_like(dqt)

    lanes = lane_iota((keys, PAIR))
    valid = key_places(keys, c * keys, 2 * rows, len_ref) < len_ref[0]
    bias = jnp.where(valid, 0.0, MASKED)
    k2 = k_ref[...].astype(jnp.float32)
    v2 = v_ref[...].astype(jnp.float32)
    kt = k2.T.astype(jnp.bfloat16)
    dv = None
    dk = None
    for h in range(2):
        mine = (lanes // HEAD_DIM) == h
        base = (1 - h) * HEAD_DIM
        ones = jnp.where((lanes >= base) & (lanes < base + 3), 1.0, 0.0)
        kx = jnp.where(mine, k2, jnp.where(lanes == base + 3, bias, ones)).astype(jnp.bfloat16)
        vx = jnp.where(mine, v2, ones).astype(jnp.bfloat16)
        s = contract_last(kx, qx[h])
        p = jnp.exp2(s * scale)
        da = contract_last(vx, gx[h])
        ds = (p * da).astype(jnp.bfloat16)
        dv_h = jnp.dot(p.astype(jnp.bfloat16), gz[h], preferred_element_type=jnp.float32)
        dk_h = jnp.dot(ds, qz[h], preferred_element_type=jnp.float32)
        dv = dv_h if dv is None else dv + dv_h
        dk = dk_h if dk is None else dk + dk_h
        half = pl.ds(h * HEAD_DIM, HEAD_DIM)
        dqt[half, :] += jnp.dot(kt[h * HEAD_DIM : (h + 1) * HEAD_DIM], ds, preferred_element_type=jnp.float32)
    root = HEAD_DIM ** -0.5
    dk_ref[...] = (dk * root).astype(jnp.bfloat16)
    dv_ref[...] = dv.astype(jnp.bfloat16)

    @pl.when(c == pl.num_programs(1) - 1)
    def _():
        dq_ref[...] = (dqt[...] * root).T.astype(jnp.bfloat16)


def attn_bwd(length, q, kv, o, lse, g, block):
    rows, width = q.shape
    keys = kv.shape[0]
    pairs = width // PAIR
    whole = pl.BlockSpec((rows, PAIR), lambda p, i, n: (0, p))
    part = pl.BlockSpec((block, PAIR), lambda p, i, n: (i, p))
    late = pl.BlockSpec((block, PAIR), lambda p, i, n: (i, pairs + p))
    out = pl.pallas_call(
        functools.partial(attn_bwd_kernel, LOG2E * HEAD_DIM ** -0.5),
        grid_spec=pltpu.PrefetchScalarGridSpec(
            num_scalar_prefetch=1,
            grid=(pairs, keys // block),
            in_specs=[whole, part, late, whole, whole, whole],
            out_specs=[whole, part, part],
            scratch_shapes=[pltpu.VMEM((2, rows, PAIR), jnp.bfloat16)] * 4
            + [pltpu.VMEM((PAIR, rows), jnp.float32)],
        ),
        out_shape=[
            jax.ShapeDtypeStruct((rows, width), jnp.bfloat16),
            jax.ShapeDtypeStruct((keys, width), jnp.bfloat16),
            jax.ShapeDtypeStruct((keys, width), jnp.bfloat16),
        ],
        name="attn_bwd",
        cost_estimate=pl.CostEstimate(flops=10 * rows * keys * width * 4, bytes_accessed=20_000_000, transcendentals=rows * keys * width // 64),
    )(length, q, kv, kv, o, lse, g)
    return out


def contract_first(a, b):
    return lax.dot_general(a, b, (((0,), (0,)), ((), ())), preferred_element_type=jnp.float32)


def dense(a, b):
    return jnp.dot(a, b, preferred_element_type=jnp.float32)


def norm_forward(values, norm_gain, norm_shift):
    centre = jnp.mean(values, axis=-1, keepdims=True)
    centred = values - centre
    inverse = lax.rsqrt(jnp.mean(centred * centred, axis=-1, keepdims=True) + 1e-06)
    normed = centred * inverse
    return (normed * norm_gain + norm_shift, normed, inverse)


def norm_backward(upstream, normed, inverse, norm_gain):
    scaled = upstream * norm_gain
    back_rows = inverse * (
        scaled
        - jnp.mean(scaled, axis=-1, keepdims=True)
        - normed * jnp.mean(scaled * normed, axis=-1, keepdims=True)
    )
    return (back_rows, jnp.sum(upstream * normed, axis=0), jnp.sum(upstream, axis=0))


def gelu_slope(values):
    return (
        0.5 * (1.0 + lax.erf(values * 0.7071067811865476))
        + values * jnp.exp(-0.5 * values * values) * 0.3989422804014327
    )


def deal(blocks):
    out = lax.all_to_all(blocks, "dp", split_axis=0, concat_axis=0, tiled=True)
    return out.reshape(-1, out.shape[-1])


def undeal(rows):
    blocks = rows.reshape(lax.axis_size("dp"), -1, rows.shape[-1])
    return lax.all_to_all(blocks, "dp", split_axis=0, concat_axis=0, tiled=True)[:, None]


def swap(value):
    return lax.ppermute(value, "tensor", [(0, 1), (1, 0)])


def in_order(own, other, axis):
    first = lax.axis_index("tensor") == 0
    return jnp.concatenate(
        [jnp.where(first, own, other), jnp.where(first, other, own)], axis=axis
    )


def join(grads):
    widths = [g.shape[1] // 2 for g in grads]
    joined = jnp.concatenate([g.astype(jnp.bfloat16) for g in grads], axis=1)
    return joined, widths


def finish_sum(joined, widths):
    part = lax.psum_scatter(joined, "dp", scatter_dimension=0, tiled=True)
    part = part.astype(jnp.float32)
    first = lax.axis_index("tensor") == 0
    left, right, start = [], [], 0
    for w in widths:
        left.append(part[:, start : start + w])
        right.append(part[:, start + w : start + 2 * w])
        start += 2 * w
    left = jnp.concatenate(left, axis=1)
    right = jnp.concatenate(right, axis=1)
    return jnp.where(first, left, right) + swap(jnp.where(first, right, left))


def per_device(
    x_in, cotangent, lengths, dealing, w_qkv, w_out, w_in, w_ffo,
    b_qv, b_out, b_in, b_ffo, ln1_gain, ln1_bias, ln2_gain, ln2_bias,
):
    low = jnp.bfloat16
    tensor_index = lax.axis_index("tensor")
    width = x_in.shape[-1]
    length = lengths[dealing[lax.axis_index("dp")]].astype(jnp.int32)
    shard = w_out.shape[0]
    local = jnp.concatenate([w.reshape(shard, -1) for w in (w_qkv, w_out, w_in, w_ffo)], axis=1)
    local = local.astype(low)
    other = swap(local)
    cuts = [0]
    for w in (w_qkv[:, 0], w_qkv[:, 1], w_qkv[:, 2], w_out, w_in, w_ffo):
        cuts.append(cuts[-1] + w.shape[1])
    pieces = [in_order(local[:, i:j], other[:, i:j], 1) for i, j in zip(cuts[:-1], cuts[1:])]
    qkv_weight = lax.all_gather(
        jnp.concatenate(pieces[:3], axis=1), "dp", axis=0, tiled=True
    )
    late_weight = lax.all_gather(jnp.concatenate(pieces[3:], axis=1), "dp", axis=0, tiled=True)
    hidden_width = 2 * w_in.shape[1]
    out_weight = late_weight[:, :width]
    in_weight = late_weight[:, width : width + hidden_width]
    ffo_weight = late_weight[:, width + hidden_width :]
    biases = jnp.concatenate([b_qv.reshape(-1), b_in])
    other = swap(biases)
    split = b_qv.shape[1]
    qv_bias = [
        in_order(biases[i * split : (i + 1) * split], other[i * split : (i + 1) * split], 0)
        for i in range(2)
    ]
    in_bias = in_order(biases[2 * split :], other[2 * split :], 0)
    tokens_half = deal(x_in[:, 0])
    half_rows = tokens_half.shape[0]
    tokens_full = jnp.concatenate([tokens_half, swap(tokens_half)], axis=0)
    place = jnp.stack([length, tensor_index.astype(jnp.int32) * half_rows])
    q_weight = qkv_weight[:, :width]
    kv_weight = qkv_weight[:, width:]
    query = (dense(tokens_half, q_weight) + qv_bias[0]).astype(low)
    kv_bias = jnp.concatenate([jnp.zeros((width,), jnp.float32), qv_bias[1]])
    keyval = (dense(tokens_full, kv_weight) + kv_bias).astype(low)
    mixed, totals = attn_fwd(place, query, keyval, 256)
    attn_half = contract_last(mixed, out_weight)
    first_norm, normed_one, inverse_one = norm_forward(
        tokens_half.astype(jnp.float32) + attn_half + b_out, ln1_gain, ln1_bias
    )
    first_low = first_norm.astype(low)
    hidden = dense(first_low, in_weight) + in_bias
    active = jax.nn.gelu(hidden, approximate=False).astype(low)
    result, normed_two, inverse_two = norm_forward(
        first_norm + contract_last(active, ffo_weight) + b_ffo, ln2_gain, ln2_bias
    )
    output_grad = deal(cotangent[:, 0]).astype(jnp.float32)
    final_grad, gain_two_grad, shift_two_grad = norm_backward(
        output_grad, normed_two, inverse_two, ln2_gain
    )
    ffo_bias_grad = jnp.sum(final_grad, axis=0)
    final_low = final_grad.astype(low)
    ffo_part = contract_first(final_low, active)
    hidden_grad = (dense(final_low, ffo_weight) * gelu_slope(hidden)).astype(low)
    in_part = contract_first(first_low, hidden_grad)
    in_bias_grad = jnp.sum(hidden_grad.astype(jnp.float32), axis=0)
    first_grad = final_grad + contract_last(hidden_grad, in_weight)
    resid_grad, gain_one_grad, shift_one_grad = norm_backward(
        first_grad, normed_one, inverse_one, ln1_gain
    )
    out_bias_grad = jnp.sum(resid_grad, axis=0)
    resid_low = resid_grad.astype(low)
    late_part, widths = join([contract_first(resid_low, mixed), in_part, ffo_part])
    mixed_grad = dense(resid_low, out_weight).astype(low)
    late_part, mixed_grad = lax.optimization_barrier((late_part, mixed_grad))
    late_sum = finish_sum(late_part, widths)
    out_sum, in_sum, ffo_sum = jnp.split(
        late_sum, [w_out.shape[1], w_out.shape[1] + w_in.shape[1]], axis=1
    )
    dq, dk, dv = attn_bwd(place, query, keyval, mixed, totals, mixed_grad, 512)
    q_bias_grad = jnp.sum(dq.astype(jnp.float32), axis=0)
    v_bias_grad = jnp.sum(dv.astype(jnp.float32), axis=0)
    qkv_part, widths = join(
        [
            contract_first(tokens_half, dq),
            contract_first(tokens_full, dk),
            contract_first(tokens_full, dv),
        ]
    )
    qkv_sum = finish_sum(qkv_part, widths).reshape(w_qkv.shape)
    shared = contract_last(dk, kv_weight[:, :width]) + contract_last(dv, kv_weight[:, width:])
    own = shared[:half_rows] + swap(shared[half_rows:].astype(low)).astype(jnp.float32)
    input_grad = resid_grad + contract_last(dq, q_weight) + own
    terms = jnp.concatenate(
        [
            out_bias_grad, ffo_bias_grad, gain_one_grad, shift_one_grad,
            gain_two_grad, shift_two_grad, q_bias_grad, v_bias_grad, in_bias_grad,
        ]
    )
    sums = lax.psum(terms, ("dp", "tensor"))
    norm_sums = sums[: 6 * width].reshape(6, width)
    qv_sums = sums[6 * width : 8 * width].reshape(2, width)
    share = b_qv.shape[1]
    qv_share = lax.dynamic_slice_in_dim(qv_sums, tensor_index * share, share, 1)
    share = b_in.shape[0]
    in_share = lax.dynamic_slice_in_dim(sums[8 * width :], tensor_index * share, share, 0)
    return (
        undeal(result.astype(low)),
        undeal(input_grad.astype(low)),
        qkv_sum,
        out_sum,
        in_sum,
        ffo_sum,
        qv_share,
        norm_sums[0],
        in_share,
        norm_sums[1],
        norm_sums[2],
        norm_sums[3],
        norm_sums[4],
        norm_sums[5],
    )


def solution(mesh):
    tokens = P(None, "tensor", "dp", None)

    return jax.shard_map(
        per_device,
        mesh=mesh,
        in_specs=(
            tokens, tokens, P(), P(),
            P("dp", None, "tensor"), P("dp", "tensor"), P("dp", "tensor"), P("dp", "tensor"),
            P(None, "tensor"), P(), P("tensor"), P(), P(), P(), P(), P(),
        ),
        out_specs=(
            tokens, tokens,
            P("dp", None, "tensor"), P("dp", "tensor"), P("dp", "tensor"), P("dp", "tensor"),
            P(None, "tensor"), P(), P("tensor"), P(), P(), P(), P(), P(),
        ),
        check_vma=False,
    )
```

```python
import functools

import jax
import jax.numpy as jnp
from jax import lax
from jax.experimental import pallas as pl
from jax.experimental.pallas import tpu as pltpu
from jax.sharding import PartitionSpec as P


LOG2E = 1.4426950408889634
MASKED = -1e30
HEAD_DIM = 64
PAIR = 2 * HEAD_DIM


def contract_last(a, b):
    return lax.dot_general(a, b, (((1,), (1,)), ((), ())), preferred_element_type=jnp.float32)


def lane_iota(shape):
    return lax.broadcasted_iota(jnp.int32, shape, len(shape) - 1)


def key_places(rows, start, total, place_ref):
    spots = lax.broadcasted_iota(jnp.int32, (rows, PAIR), 0) + (start + place_ref[1])
    return jnp.where(spots >= total, spots - total, spots)


def attn_fwd_kernel(scale, len_ref, q_ref, k_ref, v_ref, o_ref, lse_ref, kx, vx):
    keys = k_ref.shape[0]
    rows = q_ref.shape[0]

    @pl.when(pl.program_id(1) == 0)
    def _():
        lanes = lane_iota((keys, PAIR))
        valid = key_places(keys, 0, keys, len_ref) < len_ref[0]
        bias = jnp.where(valid, 0.0, MASKED)
        k2 = k_ref[...].astype(jnp.float32)
        v2 = v_ref[...].astype(jnp.float32)
        for h in range(2):
            mine = (lanes // HEAD_DIM) == h
            spare = lanes == (1 - h) * HEAD_DIM
            kx[h] = jnp.where(mine, k2, jnp.where(spare, bias, 0.0)).astype(jnp.bfloat16)
            vx[h] = jnp.where(mine, v2, 1.0).astype(jnp.bfloat16)

    lanes = lane_iota((rows, PAIR))
    q2 = q_ref[...].astype(jnp.float32)
    low = lanes < HEAD_DIM
    sums, tops = [], []
    for h in range(2):
        mine = (lanes // HEAD_DIM) == h
        spare = lanes == (1 - h) * HEAD_DIM
        qx = jnp.where(mine, q2, jnp.where(spare, 1.0, 0.0)).astype(jnp.bfloat16)
        s = contract_last(qx, kx[h])
        top = jnp.max(s, axis=1, keepdims=True)
        p = jnp.exp2(s * scale - top * scale).astype(jnp.bfloat16)
        sums.append(jnp.dot(p, vx[h], preferred_element_type=jnp.float32))
        tops.append(top * scale)
    num = jnp.where(low, sums[0], sums[1])
    den = pltpu.roll(jnp.where(low, sums[1], sums[0]), HEAD_DIM, 1)
    o_ref[...] = (num / den).astype(jnp.bfloat16)
    lse_ref[...] = jnp.where(low, tops[0], tops[1]) + jnp.log2(den)


def attn_fwd(length, q, kv, block):
    rows, width = q.shape
    keys = kv.shape[0]
    pairs = width // PAIR
    return pl.pallas_call(
        functools.partial(attn_fwd_kernel, LOG2E * HEAD_DIM ** -0.5),
        grid_spec=pltpu.PrefetchScalarGridSpec(
            num_scalar_prefetch=1,
            grid=(pairs, rows // block),
            in_specs=[
                pl.BlockSpec((block, PAIR), lambda p, i, n: (i, p)),
                pl.BlockSpec((keys, PAIR), lambda p, i, n: (0, p)),
                pl.BlockSpec((keys, PAIR), lambda p, i, n: (0, pairs + p)),
            ],
            out_specs=[
                pl.BlockSpec((block, PAIR), lambda p, i, n: (i, p)),
                pl.BlockSpec((block, PAIR), lambda p, i, n: (i, p)),
            ],
            scratch_shapes=[
                pltpu.VMEM((2, keys, PAIR), jnp.bfloat16),
                pltpu.VMEM((2, keys, PAIR), jnp.bfloat16),
            ],
        ),
        out_shape=[
            jax.ShapeDtypeStruct((rows, width), jnp.bfloat16),
            jax.ShapeDtypeStruct((rows, width), jnp.float32),
        ],
        name="attn_fwd",
        cost_estimate=pl.CostEstimate(flops=4 * rows * keys * width * 4, bytes_accessed=10_000_000, transcendentals=rows * keys * width // 64),
    )(length, q, kv, kv)


def split3(x):
    a = x.astype(jnp.bfloat16).astype(jnp.float32)
    b = (x - a).astype(jnp.bfloat16).astype(jnp.float32)
    return a, b, x - a - b


def attn_bwd_kernel(scale, len_ref, q_ref, k_ref, v_ref, o_ref, lse_ref, g_ref, dq_ref, dk_ref, dv_ref, qx, gx, qz, gz, dqt):
    rows = q_ref.shape[0]
    keys = k_ref.shape[0]
    c = pl.program_id(1)

    @pl.when(c == 0)
    def _():
        lanes = lane_iota((rows, PAIR))
        q2 = q_ref[...].astype(jnp.float32)
        g2 = g_ref[...].astype(jnp.float32)
        go = g2 * o_ref[...].astype(jnp.float32)
        other = -pltpu.roll(lse_ref[...], HEAD_DIM, 1) * (1.0 / scale)
        a, b, d = split3(other)
        for h in range(2):
            mine = (lanes // HEAD_DIM) == h
            base = (1 - h) * HEAD_DIM
            delta = -jnp.sum(jnp.where(mine, go, 0.0), axis=1, keepdims=True)
            da, db, dd = split3(delta)
            ext = jnp.where(lanes == base, a, jnp.where(lanes == base + 1, b, jnp.where(lanes == base + 2, d, jnp.where(lanes == base + 3, 1.0, 0.0))))
            qx[h] = jnp.where(mine, q2, ext).astype(jnp.bfloat16)
            qz[h] = jnp.where(mine, q2, 0.0).astype(jnp.bfloat16)
            ext = jnp.where(lanes == base, da, jnp.where(lanes == base + 1, db, jnp.where(lanes == base + 2, dd, 0.0)))
            gx[h] = jnp.where(mine, g2, ext).astype(jnp.bfloat16)
            gz[h] = jnp.where(mine, g2, 0.0).astype(jnp.bfloat16)
        dqt[...] = jnp.zeros_like(dqt)

    lanes = lane_iota((keys, PAIR))
    valid = key_places(keys, c * keys, 2 * rows, len_ref) < len_ref[0]
    bias = jnp.where(valid, 0.0, MASKED)
    k2 = k_ref[...].astype(jnp.float32)
    v2 = v_ref[...].astype(jnp.float32)
    kt = k2.T.astype(jnp.bfloat16)
    dv = None
    dk = None
    for h in range(2):
        mine = (lanes // HEAD_DIM) == h
        base = (1 - h) * HEAD_DIM
        ones = jnp.where((lanes >= base) & (lanes < base + 3), 1.0, 0.0)
        kx = jnp.where(mine, k2, jnp.where(lanes == base + 3, bias, ones)).astype(jnp.bfloat16)
        vx = jnp.where(mine, v2, ones).astype(jnp.bfloat16)
        s = contract_last(kx, qx[h])
        p = jnp.exp2(s * scale)
        da = contract_last(vx, gx[h])
        ds = (p * da).astype(jnp.bfloat16)
        dv_h = jnp.dot(p.astype(jnp.bfloat16), gz[h], preferred_element_type=jnp.float32)
        dk_h = jnp.dot(ds, qz[h], preferred_element_type=jnp.float32)
        dv = dv_h if dv is None else dv + dv_h
        dk = dk_h if dk is None else dk + dk_h
        half = pl.ds(h * HEAD_DIM, HEAD_DIM)
        dqt[half, :] += jnp.dot(kt[h * HEAD_DIM : (h + 1) * HEAD_DIM], ds, preferred_element_type=jnp.float32)
    root = HEAD_DIM ** -0.5
    dk_ref[...] = (dk * root).astype(jnp.bfloat16)
    dv_ref[...] = dv.astype(jnp.bfloat16)

    @pl.when(c == pl.num_programs(1) - 1)
    def _():
        dq_ref[...] = (dqt[...] * root).T.astype(jnp.bfloat16)


def attn_bwd(length, q, kv, o, lse, g, block):
    rows, width = q.shape
    keys = kv.shape[0]
    pairs = width // PAIR
    whole = pl.BlockSpec((rows, PAIR), lambda p, i, n: (0, p))
    part = pl.BlockSpec((block, PAIR), lambda p, i, n: (i, p))
    late = pl.BlockSpec((block, PAIR), lambda p, i, n: (i, pairs + p))
    out = pl.pallas_call(
        functools.partial(attn_bwd_kernel, LOG2E * HEAD_DIM ** -0.5),
        grid_spec=pltpu.PrefetchScalarGridSpec(
            num_scalar_prefetch=1,
            grid=(pairs, keys // block),
            in_specs=[whole, part, late, whole, whole, whole],
            out_specs=[whole, part, part],
            scratch_shapes=[pltpu.VMEM((2, rows, PAIR), jnp.bfloat16)] * 4
            + [pltpu.VMEM((PAIR, rows), jnp.float32)],
        ),
        out_shape=[
            jax.ShapeDtypeStruct((rows, width), jnp.bfloat16),
            jax.ShapeDtypeStruct((keys, width), jnp.bfloat16),
            jax.ShapeDtypeStruct((keys, width), jnp.bfloat16),
        ],
        name="attn_bwd",
        cost_estimate=pl.CostEstimate(flops=10 * rows * keys * width * 4, bytes_accessed=20_000_000, transcendentals=rows * keys * width // 64),
    )(length, q, kv, kv, o, lse, g)
    return out


def contract_first(a, b):
    return lax.dot_general(a, b, (((0,), (0,)), ((), ())), preferred_element_type=jnp.float32)


def dense(a, b):
    return jnp.dot(a, b, preferred_element_type=jnp.float32)


def norm_forward(values, norm_gain, norm_shift):
    centre = jnp.mean(values, axis=-1, keepdims=True)
    centred = values - centre
    inverse = lax.rsqrt(jnp.mean(centred * centred, axis=-1, keepdims=True) + 1e-06)
    normed = centred * inverse
    return (normed * norm_gain + norm_shift, normed, inverse)


def norm_backward(upstream, normed, inverse, norm_gain):
    scaled = upstream * norm_gain
    back_rows = inverse * (
        scaled
        - jnp.mean(scaled, axis=-1, keepdims=True)
        - normed * jnp.mean(scaled * normed, axis=-1, keepdims=True)
    )
    return (back_rows, jnp.sum(upstream * normed, axis=0), jnp.sum(upstream, axis=0))


def gelu_slope(values):
    return (
        0.5 * (1.0 + lax.erf(values * 0.7071067811865476))
        + values * jnp.exp(-0.5 * values * values) * 0.3989422804014327
    )


def mesh_copy(src, dst, send_sem, recv_sem, dp, tensor):
    return pltpu.make_async_remote_copy(
        src_ref=src,
        dst_ref=dst,
        send_sem=send_sem,
        recv_sem=recv_sem,
        device_id={"dp": dp, "tensor": tensor},
        device_id_type=pl.DeviceIdType.MESH,
    )


def greet_all(n, me, side):
    barrier = pltpu.get_barrier_semaphore()

    def greet(step, carry):
        pl.semaphore_signal(
            barrier,
            inc=1,
            device_id={"dp": lax.rem(me + step, n), "tensor": side},
            device_id_type=pl.DeviceIdType.MESH,
        )
        return carry

    lax.fori_loop(1, n, greet, 0)
    pl.semaphore_signal(
        barrier,
        inc=1,
        device_id={"dp": me, "tensor": 1 - side},
        device_id_type=pl.DeviceIdType.MESH,
    )
    pl.semaphore_wait(barrier, n)


def repeat(low, high, body):
    def step_body(step, carry):
        body(step)
        return carry

    lax.fori_loop(low, high, step_body, 0)


def deal_kernel(n, x_ref, o_ref, send, recv, relay_send, relay_recv):
    me, side = lax.axis_index("dp"), lax.axis_index("tensor")
    greet_all(n, me, side)

    def direct(step):
        dest = lax.rem(me + step, n)
        return mesh_copy(
            x_ref.at[dest], o_ref.at[0, me], send.at[step], recv.at[step], dest, side
        )

    def arrival(step):
        src = lax.rem(me + n - step, n)
        return mesh_copy(
            x_ref.at[src], o_ref.at[0, src], send.at[step], recv.at[step], src, side
        )

    def relay(step):
        src = lax.rem(me + n - step, n)
        return mesh_copy(
            o_ref.at[0, src], o_ref.at[1, src], relay_send.at[step], relay_recv.at[step],
            me, 1 - side,
        )

    repeat(1, n, lambda step: direct(step).start())
    first = mesh_copy(
        x_ref.at[me], o_ref.at[1, me], relay_send.at[0], relay_recv.at[0], me, 1 - side
    )
    first.start()
    o_ref[0, me] = x_ref[me]

    def pass_on(step):
        arrival(step).wait_recv()
        relay(step).start()

    repeat(1, n, pass_on)

    def finish(step):
        direct(step).wait_send()
        relay(step).wait()

    repeat(1, n, finish)
    first.wait()


def deal_both(blocks):
    n, rows, width = blocks.shape
    vmem = pl.BlockSpec(memory_space=pltpu.VMEM)
    out = pl.pallas_call(
        functools.partial(deal_kernel, n),
        out_shape=jax.ShapeDtypeStruct((2, n, rows, width), blocks.dtype),
        in_specs=[vmem],
        out_specs=vmem,
        scratch_shapes=[pltpu.SemaphoreType.DMA((n,))] * 4,
        compiler_params=pltpu.CompilerParams(collective_id=0, has_side_effects=True),
        name="deal_both",
    )(blocks)
    return out.reshape(2 * n * rows, width)


def settle_kernel(
    n, own_ref, far_ref, terms_ref, out_ref, sums_ref, inbox, stage, their, pair, pile, total,
    a_send, a_recv, y_send, y_recv, b_send, b_recv, c_send, c_recv, d_send, d_recv,
):
    me, side = lax.axis_index("dp"), lax.axis_index("tensor")
    greet_all(n, me, side)
    whole = mesh_copy(terms_ref, their, a_send, a_recv, me, 1 - side)
    whole.start()

    def across(step):
        dest = lax.rem(me + step, n)
        return mesh_copy(
            far_ref.at[dest], inbox.at[dest], y_send.at[step], y_recv.at[step], me, 1 - side
        )

    def home(step, src_side):
        dest = lax.rem(me + step, n)
        src = lax.rem(me + n - step, n)
        where = src if src_side else me
        return mesh_copy(
            stage.at[dest], out_ref.at[where], d_send.at[step], d_recv.at[step], dest, side
        )

    def chunk(step, src_side):
        dest = lax.rem(me + step, n)
        src = lax.rem(me + n - step, n)
        where = src if src_side else me
        return mesh_copy(
            pair.at[dest], pile.at[where], b_send.at[step], b_recv.at[step], dest, side
        )

    def share(step, src_side):
        dest = lax.rem(me + step, n)
        src = lax.rem(me + n - step, n)
        where = src if src_side else me
        return mesh_copy(
            total, sums_ref.at[where], c_send.at[step], c_recv.at[step], dest, side
        )

    repeat(1, n, lambda step: across(step).start())
    across(0).start()
    whole.wait()
    pair[...] = terms_ref[...] + their[...]
    pile[me] = pair[me]

    def add(step):
        across(step).wait_recv()
        dest = lax.rem(me + step, n)
        stage[dest] = (own_ref[dest] + inbox[dest].astype(jnp.float32)).astype(stage.dtype)

    add(1)
    repeat(1, n, lambda step: chunk(step, False).start())

    def move(step):
        add(step)
        home(step - 1, False).start()

    repeat(2, n, move)
    across(0).wait_recv()
    out_ref[me] = (own_ref[me] + inbox[me].astype(jnp.float32)).astype(out_ref.dtype)
    home(n - 1, False).start()
    repeat(1, n, lambda step: chunk(step, True).wait_recv())
    total[...] = jnp.sum(pile[...], axis=0)
    sums_ref[me] = total[...]
    repeat(1, n, lambda step: home(step, True).wait_recv())
    repeat(1, n, lambda step: share(step, False).start())

    def finish(step):
        share(step, True).wait_recv()
        share(step, False).wait_send()
        home(step, False).wait_send()
        chunk(step, False).wait_send()
        across(step).wait_send()

    repeat(1, n, finish)
    across(0).wait_send()


def settle(own, far, terms):
    n = lax.axis_size("dp")
    rows, width = own.shape
    per = rows // n
    lines = 8 * -(-terms.shape[0] // (n * 1024))
    padded = jnp.pad(terms, (0, n * lines * 128 - terms.shape[0])).reshape(n, lines, 128)
    vmem = pl.BlockSpec(memory_space=pltpu.VMEM)
    low = jnp.bfloat16
    blocks = (n, per, width)
    out, sums = pl.pallas_call(
        functools.partial(settle_kernel, n),
        out_shape=[
            jax.ShapeDtypeStruct(blocks, low),
            jax.ShapeDtypeStruct(padded.shape, jnp.float32),
        ],
        in_specs=[vmem] * 3,
        out_specs=[vmem] * 2,
        scratch_shapes=[
            pltpu.VMEM(blocks, low),
            pltpu.VMEM(blocks, low),
            pltpu.VMEM(padded.shape, jnp.float32),
            pltpu.VMEM(padded.shape, jnp.float32),
            pltpu.VMEM(padded.shape, jnp.float32),
            pltpu.VMEM((lines, 128), jnp.float32),
            pltpu.SemaphoreType.DMA,
            pltpu.SemaphoreType.DMA,
        ]
        + [pltpu.SemaphoreType.DMA((n,))] * 8,
        compiler_params=pltpu.CompilerParams(collective_id=1, has_side_effects=True),
        name="settle",
    )(own.reshape(blocks), far.reshape(blocks), padded)
    return out[:, None], sums.reshape(-1)[: terms.shape[0]]


def deal(blocks):
    out = lax.all_to_all(blocks, "dp", split_axis=0, concat_axis=0, tiled=True)
    return out.reshape(-1, out.shape[-1])


def undeal(rows):
    blocks = rows.reshape(lax.axis_size("dp"), -1, rows.shape[-1])
    return lax.all_to_all(blocks, "dp", split_axis=0, concat_axis=0, tiled=True)[:, None]


def swap(value):
    return lax.ppermute(value, "tensor", [(0, 1), (1, 0)])


def in_order(own, other, axis):
    first = lax.axis_index("tensor") == 0
    return jnp.concatenate(
        [jnp.where(first, own, other), jnp.where(first, other, own)], axis=axis
    )


def join(grads):
    widths = [g.shape[1] // 2 for g in grads]
    joined = jnp.concatenate([g.astype(jnp.bfloat16) for g in grads], axis=1)
    return joined, widths


def finish_sum(joined, widths):
    part = lax.psum_scatter(joined, "dp", scatter_dimension=0, tiled=True)
    part = part.astype(jnp.float32)
    first = lax.axis_index("tensor") == 0
    left, right, start = [], [], 0
    for w in widths:
        left.append(part[:, start : start + w])
        right.append(part[:, start + w : start + 2 * w])
        start += 2 * w
    left = jnp.concatenate(left, axis=1)
    right = jnp.concatenate(right, axis=1)
    return jnp.where(first, left, right) + swap(jnp.where(first, right, left))


def per_device(
    x_in, cotangent, lengths, dealing, w_qkv, w_out, w_in, w_ffo,
    b_qv, b_out, b_in, b_ffo, ln1_gain, ln1_bias, ln2_gain, ln2_bias,
):
    low = jnp.bfloat16
    tensor_index = lax.axis_index("tensor")
    width = x_in.shape[-1]
    length = lengths[dealing[lax.axis_index("dp")]].astype(jnp.int32)

    def paired(weights):
        local = jnp.concatenate([w.astype(low) for w in weights], axis=1)
        other = swap(local)
        cuts = [0]
        for w in weights:
            cuts.append(cuts[-1] + w.shape[1])
        pieces = [in_order(local[:, i:j], other[:, i:j], 1) for i, j in zip(cuts[:-1], cuts[1:])]
        return jnp.concatenate(pieces, axis=1)

    qkv_weight = lax.all_gather(
        paired([w_qkv[:, 0], w_qkv[:, 1], w_qkv[:, 2]]), "dp", axis=0, tiled=True
    )
    late_weight = lax.all_gather(paired([w_out, w_in, w_ffo]), "dp", axis=0, tiled=True)
    hidden_width = 2 * w_in.shape[1]
    out_weight = late_weight[:, :width]
    in_weight = late_weight[:, width : width + hidden_width]
    ffo_weight = late_weight[:, width + hidden_width :]
    biases = jnp.concatenate([b_qv.reshape(-1), b_in])
    other = swap(biases)
    split = b_qv.shape[1]
    qv_bias = [
        in_order(biases[i * split : (i + 1) * split], other[i * split : (i + 1) * split], 0)
        for i in range(2)
    ]
    in_bias = in_order(biases[2 * split :], other[2 * split :], 0)
    tokens_full = deal_both(x_in[:, 0])
    half_rows = tokens_full.shape[0] // 2
    tokens_half = tokens_full[:half_rows]
    tokens_full, cotangent = lax.optimization_barrier((tokens_full, cotangent))
    output_grad = deal(cotangent[:, 0]).astype(jnp.float32)
    place = jnp.stack([length, tensor_index.astype(jnp.int32) * half_rows])
    q_weight = qkv_weight[:, :width]
    kv_weight = qkv_weight[:, width:]
    query = (dense(tokens_half, q_weight) + qv_bias[0]).astype(low)
    kv_bias = jnp.concatenate([jnp.zeros((width,), jnp.float32), qv_bias[1]])
    keyval = (dense(tokens_full, kv_weight) + kv_bias).astype(low)
    mixed, totals = attn_fwd(place, query, keyval, 256)
    attn_half = contract_last(mixed, out_weight)
    first_norm, normed_one, inverse_one = norm_forward(
        tokens_half.astype(jnp.float32) + attn_half + b_out, ln1_gain, ln1_bias
    )
    first_low = first_norm.astype(low)
    hidden = dense(first_low, in_weight) + in_bias
    active = jax.nn.gelu(hidden, approximate=False).astype(low)
    result, normed_two, inverse_two = norm_forward(
        first_norm + contract_last(active, ffo_weight) + b_ffo, ln2_gain, ln2_bias
    )
    final_grad, gain_two_grad, shift_two_grad = norm_backward(
        output_grad, normed_two, inverse_two, ln2_gain
    )
    ffo_bias_grad = jnp.sum(final_grad, axis=0)
    final_low = final_grad.astype(low)
    ffo_part = contract_first(final_low, active)
    hidden_grad = (dense(final_low, ffo_weight) * gelu_slope(hidden)).astype(low)
    in_part = contract_first(first_low, hidden_grad)
    in_bias_grad = jnp.sum(hidden_grad.astype(jnp.float32), axis=0)
    first_grad = final_grad + contract_last(hidden_grad, in_weight)
    resid_grad, gain_one_grad, shift_one_grad = norm_backward(
        first_grad, normed_one, inverse_one, ln1_gain
    )
    out_bias_grad = jnp.sum(resid_grad, axis=0)
    resid_low = resid_grad.astype(low)
    late_part, widths = join([contract_first(resid_low, mixed), in_part, ffo_part])
    mixed_grad = dense(resid_low, out_weight).astype(low)
    late_part, mixed_grad = lax.optimization_barrier((late_part, mixed_grad))
    late_sum = finish_sum(late_part, widths)
    out_sum, in_sum, ffo_sum = jnp.split(
        late_sum, [w_out.shape[1], w_out.shape[1] + w_in.shape[1]], axis=1
    )
    dq, dk, dv = attn_bwd(place, query, keyval, mixed, totals, mixed_grad, 512)
    q_bias_grad = jnp.sum(dq.astype(jnp.float32), axis=0)
    v_bias_grad = jnp.sum(dv.astype(jnp.float32), axis=0)
    qkv_part, widths = join(
        [
            contract_first(tokens_half, dq),
            contract_first(tokens_full, dk),
            contract_first(tokens_full, dv),
        ]
    )
    qkv_sum = finish_sum(qkv_part, widths).reshape(w_qkv.shape)
    shared = contract_last(dk, kv_weight[:, :width]) + contract_last(dv, kv_weight[:, width:])
    own = resid_grad + contract_last(dq, q_weight) + shared[:half_rows]
    terms = jnp.concatenate(
        [
            out_bias_grad, ffo_bias_grad, gain_one_grad, shift_one_grad,
            gain_two_grad, shift_two_grad, q_bias_grad, v_bias_grad, in_bias_grad,
        ]
    )
    input_grad, sums = settle(own, shared[half_rows:].astype(low), terms)
    norm_sums = sums[: 6 * width].reshape(6, width)
    qv_sums = sums[6 * width : 8 * width].reshape(2, width)
    share = b_qv.shape[1]
    qv_share = lax.dynamic_slice_in_dim(qv_sums, tensor_index * share, share, 1)
    share = b_in.shape[0]
    in_share = lax.dynamic_slice_in_dim(sums[8 * width :], tensor_index * share, share, 0)
    output = undeal(result.astype(low))
    return (
        output,
        input_grad,
        qkv_sum,
        out_sum,
        in_sum,
        ffo_sum,
        qv_share,
        norm_sums[0],
        in_share,
        norm_sums[1],
        norm_sums[2],
        norm_sums[3],
        norm_sums[4],
        norm_sums[5],
    )


def solution(mesh):
    tokens = P(None, "tensor", "dp", None)

    return jax.shard_map(
        per_device,
        mesh=mesh,
        in_specs=(
            tokens, tokens, P(), P(),
            P("dp", None, "tensor"), P("dp", "tensor"), P("dp", "tensor"), P("dp", "tensor"),
            P(None, "tensor"), P(), P("tensor"), P(), P(), P(), P(), P(),
        ),
        out_specs=(
            tokens, tokens,
            P("dp", None, "tensor"), P("dp", "tensor"), P("dp", "tensor"), P("dp", "tensor"),
            P(None, "tensor"), P(), P("tensor"), P(), P(), P(), P(), P(),
        ),
        check_vma=False,
    )
```
